32 devices in a mesh: slab: 4 (over y, x), blk: 8 (over z, core).
Axes of the slice: x: 2, y: 2, z: 4, core: 2. Of those that a mesh axis runs over, the one named last changes fastest.
Arguments:
- amplitudes: bfloat16 [32, 3, 56, 128, 128], P('slab', None, 'blk'), may hold values from -6 to 6
- integrals: bfloat16 [32, 3, 1200, 1200], P(('slab', 'blk')), may hold values from -0.03125 to 0.03125
- slot_tile: int32 [56], replicated, may hold values from -1 to 99, as said below
Outputs:
- residual: float32 [3, 56, 128, 128], P(None, 'blk', 'slab')
The draws below stay inside these ranges and needn't reach their ends.
Inputs may be any that keep to these rules, and one draw needn't show every extreme that they name: `slot_tile`: each of the 55 block pairs x * 10 + y with x <= y is named by exactly one slot; every other slot holds -1.
All inputs are finite; a program needn't handle non-finite values.
Results may differ from the reference program's by a relative error of at most 0.0003.
Values may be sent and summed in bfloat16 or wider, within the bound.
A program may use at most 128 MiB of HBM per device.

```python
import jax
import jax.numpy as jnp
import numpy as np
from jax import lax

V = 1200
TILE = 128
NOUT = 3
K = 32
VB = 10
VP = 1280
NTILE = 55
SLOTS = 56


def draw_slot_tile(key, part):
    listing = [x_blk * VB + y_blk for x_blk in range(VB) for y_blk in range(x_blk, VB)]
    listing = listing + [-1] * (SLOTS - NTILE)
    table = jnp.asarray(np.array(listing, dtype=np.int32))
    placing = jax.random.permutation(key, SLOTS)
    return jnp.zeros((SLOTS,), jnp.int32).at[placing].set(table).astype(jnp.int32)


def block_scale(own_key, shape, split, least, largest):
    loudness, own = 1.0, jax.random.fold_in(own_key, 6)
    for axis_at, shards_of in split:
        heights = jnp.exp(jax.random.uniform(jax.random.fold_in(own, axis_at), (shards_of,), jnp.float32, least / len(split), largest / len(split)))
        loudness = loudness * jnp.repeat(heights, shape[axis_at] // shards_of).reshape([-1 if axis == axis_at else 1 for axis in range(len(shape))])
    return loudness


def bell_draw(rng, shape, spread, limit, cuts=(), kind=jnp.bfloat16):
    factor_of = block_scale(rng, shape, cuts, -0.22, 0.18) if cuts else 1.0
    drawn = jax.random.normal(rng, shape, jnp.float32) * spread * factor_of
    return jnp.minimum(jnp.maximum(drawn, -limit), limit).astype(kind)


def setup_inputs(seed: int = 0) -> dict:
    key_list = jax.random.split(jax.random.key(seed), 4)
    amplitudes = bell_draw(key_list[0], (K, NOUT, SLOTS, TILE, TILE), 1.0, 6.0, ((0, 4), (2, 8)))
    integrals = bell_draw(key_list[1], (K, NOUT, V, V), (K * V) ** -0.5, 0.03125, ((0, 32),))
    slot_tile = draw_slot_tile(jax.random.fold_in(key_list[3], 71), 0)
    return dict(amplitudes=amplitudes, integrals=integrals, slot_tile=slot_tile)


def strict_upper(tile_len):
    row_ids = jnp.arange(tile_len)[:, None]
    col_ids = jnp.arange(tile_len)[None, :]
    return row_ids < col_ids


def unpack(packed, slot_tile):
    tile_ids = jnp.arange(VB * VB, dtype=jnp.int32)
    matches = slot_tile[None, :] == tile_ids[:, None]
    slot_ids = jnp.arange(SLOTS, dtype=jnp.int32)[None, :]
    slot_of = jnp.sum(jnp.where(matches, slot_ids, 0), axis=1).astype(jnp.int32)
    present = jnp.any(matches, axis=1)
    tiles = jnp.where(present[:, None, None], packed[slot_of], jnp.zeros((), packed.dtype))
    on_diag = (tile_ids // VB) == (tile_ids % VB)
    keeping = jnp.logical_or(jnp.logical_not(on_diag)[:, None, None], strict_upper(TILE)[None])
    tiles = jnp.where(keeping, tiles, jnp.zeros((), packed.dtype))
    whole = tiles.reshape(VB, VB, TILE, TILE).transpose(0, 2, 1, 3).reshape(VP, VP)
    return (whole - whole.T)[:V, :V]


def reference(amplitudes, integrals, slot_tile):
    ordered = [(source, target) for source in range(NOUT) for target in range(NOUT) if source != target]

    def advance(carry, inputs):
        amp_slab, int_slab = inputs
        fulls = [unpack(amp_slab[source], slot_tile) for source in range(NOUT)]
        updated = tuple(
            carry[number] + jnp.dot(fulls[pair[0]], int_slab[pair[1]], preferred_element_type=jnp.float32)
            for number, pair in enumerate(ordered)
        )
        return updated, None

    initial = tuple(jnp.zeros((V, V), jnp.float32) for entry in ordered)
    sums = lax.scan(advance, initial, (amplitudes, integrals))[0]
    lookup = {pair: number for number, pair in enumerate(ordered)}
    safe_ids = jnp.clip(slot_tile, 0, VB * VB - 1).astype(jnp.int32)
    present = (slot_tile >= 0)[:, None, None]
    results = []
    for source in range(NOUT):
        for target in range(source + 1, NOUT):
            differ = sums[lookup[(source, target)]] - sums[lookup[(target, source)]]
            resid = differ - differ.T
            padded = jnp.pad(resid, ((0, VP - V), (0, VP - V)))
            tiles = padded.reshape(VB, TILE, VB, TILE).transpose(0, 2, 1, 3).reshape(VB * VB, TILE, TILE)
            results.append(jnp.where(present, tiles[safe_ids], jnp.zeros((), jnp.float32)))
    return jnp.stack(results).astype(jnp.float32)
```

```python
import functools

import jax
import jax.numpy as jnp
from jax import lax
from jax.experimental import pallas as pl
from jax.experimental.pallas import tpu as pltpu
from jax.sharding import PartitionSpec as P

MESH = pl.DeviceIdType.MESH


def flip(index, mask):
    out = index
    bit = 1
    while bit <= mask:
        if mask & bit:
            out = out + bit * (1 - 2 * ((index // bit) % 2))
        bit *= 2
    return out


def row_chunk(rows):
    return max(size for size in range(16, 257, 16) if rows % size == 0)


def cycle_kernel(
    dims,
    from_ref, tile_ref, amp_ref, int_ref, out_ref,
    packed0, packed1, packed2, full0, full1, full2, landing, weights, acc_a, acc_b,
    outgoing, mates, first_in, second_in, last_in,
    load_sem, local_sem, amp_send, amp_recv, mate_send, mate_recv,
    first_send, first_recv, second_send, second_recv, last_send, last_recv,
):
    n_slab, n_blk, blocks, v_width, slot_dev, tile_len = dims
    n_z = n_blk // 2
    half_z = n_z // 2
    padded = blocks * tile_len
    row_part = tile_len // n_slab
    n_slots = n_blk * slot_dev
    packed = (packed0, packed1, packed2)
    fulls = (full0, full1, full2)
    slab = lax.axis_index("slab")
    blk = lax.axis_index("blk")
    core = blk % 2
    z_at = blk // 2

    barrier = pltpu.get_barrier_semaphore()
    for mask in range(1, n_blk):
        pl.semaphore_signal(barrier, inc=1, device_id={"blk": flip(blk, mask)}, device_id_type=MESH)
    for mask in (1, 2):
        pl.semaphore_signal(barrier, inc=1, device_id={"slab": flip(slab, mask)}, device_id_type=MESH)
    pl.semaphore_wait(barrier, n_blk + 1)

    def amp_copy(which, mask):
        target = flip(blk, mask)
        return pltpu.make_async_remote_copy(
            src_ref=amp_ref.at[target, which],
            dst_ref=packed[which].at[blk],
            send_sem=amp_send.at[which, mask],
            recv_sem=amp_recv.at[which, mask],
            device_id={"blk": target},
            device_id_type=MESH,
        )

    def own_copy(which):
        return pltpu.make_async_copy(amp_ref.at[blk, which], packed[which].at[blk], local_sem.at[which])

    for which in range(3):
        for mask in reversed(range(1, n_blk)):
            amp_copy(which, mask).start()
        own_copy(which).start()

    chunk = landing.shape[1]
    n_chunk = v_width // chunk
    pad = padded - v_width

    def int_copy(number):
        which, at = divmod(number, n_chunk)
        return pltpu.make_async_copy(
            int_ref.at[0, which, pl.ds(at * chunk, chunk)], landing.at[number % 2], load_sem.at[number % 2]
        )

    int_copy(0).start()
    for number in range(3 * n_chunk):
        which, at = divmod(number, n_chunk)
        if number + 1 < 3 * n_chunk:
            int_copy(number + 1).start()
        int_copy(number).wait()
        weights[which, pl.ds(at * chunk, chunk), pl.ds(0, v_width)] = landing[number % 2]
    if pad:
        for which in range(3):
            weights[which, :, pl.ds(v_width, pad)] = jnp.zeros((padded, pad), weights.dtype)
            weights[which, pl.ds(v_width, pad), :] = jnp.zeros((pad, padded), weights.dtype)

    row_ids = lax.broadcasted_iota(jnp.int32, (tile_len, tile_len), 0)
    col_ids = lax.broadcasted_iota(jnp.int32, (tile_len, tile_len), 1)

    def put_tile(which, x, y):
        at = x * blocks + y
        rows = pl.ds(pl.multiple_of(x * tile_len, tile_len), tile_len)
        cols = pl.ds(pl.multiple_of(y * tile_len, tile_len), tile_len)
        keep = jnp.logical_and(row_ids + x * tile_len < col_ids + y * tile_len, col_ids + y * tile_len < v_width)
        raw = packed[which][from_ref[0, at], from_ref[1, at]]
        tile = jnp.where(keep, raw.astype(jnp.float32), 0.0)
        mirror = tile.T
        same = jnp.where(x == y, 1.0, 0.0)
        fulls[which][rows, cols] = (tile - same * mirror).astype(raw.dtype)
        fulls[which][cols, rows] = (same * tile - mirror).astype(raw.dtype)

    def build(which):
        for mask in range(1, n_blk):
            amp_copy(which, mask).wait_recv()
        own_copy(which).wait()
        if blocks % 2:
            for x in range(blocks):
                for y in range(x, blocks):
                    put_tile(which, x, y)
            return

        def fold(i, carry):
            for j in range(blocks + 1):
                upper = j < blocks - i
                x = jnp.where(upper, i, blocks - 1 - i)
                y = jnp.where(upper, i + j, j - 1)
                put_tile(which, x, y)
            return carry

        lax.fori_loop(0, blocks // 2, fold, 0)

    width = 2 * tile_len if padded % (2 * tile_len) == 0 else tile_len

    per_step = width // tile_len

    def product(left, right, cols):
        return jnp.dot(fulls[left][...], weights[right, :, cols], preferred_element_type=jnp.float32)

    def by_columns(acc, fresh, terms):
        def step(number, carry):
            cols = pl.ds(pl.multiple_of(number * width, width), width)
            total = None
            for sign, left, right in terms:
                term = product(left, right, cols)
                total = (term if sign > 0 else -term) if total is None else total + term if sign > 0 else total - term
            for x in range(blocks):
                for part in range(per_step):
                    y = number * per_step + part
                    tile = total[x * tile_len : (x + 1) * tile_len, part * tile_len : (part + 1) * tile_len]
                    acc[x, y] = tile if fresh else acc[x, y] + tile
            return carry

        lax.fori_loop(0, padded // width, step, 0)

    def pack(acc):
        def owner_tiles(owner, carry):
            for place in range(slot_dev):
                slot = owner * slot_dev + place
                first, second, used = tile_ref[0, slot], tile_ref[1, slot], tile_ref[2, slot]
                tile = (acc[first, second] - acc[second, first].T) * used.astype(jnp.float32)
                for part in range(n_slab):
                    outgoing[owner % 2, part, owner // 2, place] = tile[part * row_part : (part + 1) * row_part]
            return carry

        lax.fori_loop(0, n_blk, owner_tiles, 0)

    def mate_copy(pair, mask):
        part = flip(slab, mask)
        return pltpu.make_async_remote_copy(
            src_ref=outgoing.at[1 - core, part],
            dst_ref=mates.at[pair, part],
            send_sem=mate_send.at[pair, mask],
            recv_sem=mate_recv.at[pair, mask],
            device_id={"blk": flip(blk, 1)},
            device_id_type=MESH,
        )

    halves = (pl.ds(0, half_z), pl.ds(half_z, n_z - half_z))

    def first_copy(pair, half, far):
        mine, other = (1, 2) if half == 0 else (2, 1)
        part = flip(slab, 3 if far else mine)
        return pltpu.make_async_remote_copy(
            src_ref=mates.at[pair, part, halves[half]],
            dst_ref=first_in.at[pair, half, far],
            send_sem=first_send.at[pair, half, far],
            recv_sem=first_recv.at[pair, half, far],
            device_id={"slab": flip(slab, mine)},
            device_id_type=MESH,
        )

    def second_copy(pair, half):
        other = 2 if half == 0 else 1
        return pltpu.make_async_remote_copy(
            src_ref=mates.at[pair, flip(slab, other), halves[half]],
            dst_ref=second_in.at[pair, half],
            send_sem=second_send.at[pair, half],
            recv_sem=second_recv.at[pair, half],
            device_id={"slab": flip(slab, other)},
            device_id_type=MESH,
        )

    def last_copy(pair, mask):
        target = flip(z_at, mask)
        return pltpu.make_async_remote_copy(
            src_ref=mates.at[pair, slab, target],
            dst_ref=last_in.at[pair, mask],
            send_sem=last_send.at[pair, mask],
            recv_sem=last_recv.at[pair, mask],
            device_id={"blk": target * 2 + core},
            device_id_type=MESH,
        )

    def mates_start(pair):
        for mask in (3, 1, 2, 0):
            mate_copy(pair, mask).start()

    def mates_finish(pair):
        for mask in (3, 1, 2, 0):
            mate_copy(pair, mask).wait_recv()
            part = flip(slab, mask)
            mates[pair, part] = mates[pair, part] + outgoing[core, part]
            if mask == 3:
                first_copy(pair, 0, 1).start()
                first_copy(pair, 1, 1).start()
            if mask == 1:
                first_copy(pair, 0, 0).start()
            if mask == 2:
                first_copy(pair, 1, 0).start()
        for mask in (3, 1, 2, 0):
            mate_copy(pair, mask).wait_send()

    def first_finish(pair):
        for half in (0, 1):
            part = flip(slab, 2 if half == 0 else 1)
            first_copy(pair, half, 1).wait_recv()
            mates[pair, part, halves[half]] = mates[pair, part, halves[half]] + first_in[pair, half, 1]
            second_copy(pair, half).start()

    def second_finish(pair):
        for half in (0, 1):
            first_copy(pair, half, 0).wait_recv()
            second_copy(pair, half).wait_recv()
            mates[pair, slab, halves[half]] = (
                mates[pair, slab, halves[half]] + first_in[pair, half, 0] + second_in[pair, half]
            )

    def last_start(pair):
        for mask in reversed(range(1, n_z)):
            last_copy(pair, mask).start()

    def last_finish(pair):
        total = mates[pair, slab, z_at]
        for mask in range(1, n_z):
            last_copy(pair, mask).wait_recv()
            total = total + last_in[pair, mask]
        out_ref[pair] = total

    pair01, pair02, pair12 = 0, 1, 2
    build(0)
    build(1)

    by_columns(acc_a, True, ((1, 0, 1), (-1, 1, 0)))
    pack(acc_a)
    mates_start(pair01)

    by_columns(acc_b, True, ((1, 0, 2),))
    mates_finish(pair01)

    by_columns(acc_a, True, ((1, 1, 2),))
    first_finish(pair01)
    second_finish(pair01)

    build(2)
    last_start(pair01)

    by_columns(acc_b, False, ((-1, 2, 0),))
    pack(acc_b)
    mates_start(pair02)

    by_columns(acc_a, False, ((-1, 2, 1),))
    mates_finish(pair02)
    pack(acc_a)
    mates_start(pair12)
    mates_finish(pair12)
    first_finish(pair02)
    second_finish(pair02)
    last_start(pair02)
    first_finish(pair12)
    last_finish(pair01)
    second_finish(pair12)
    last_start(pair12)
    last_finish(pair02)
    last_finish(pair12)

    for which in range(3):
        for mask in range(1, n_blk):
            amp_copy(which, mask).wait_send()
    for pair in (pair01, pair02, pair12):
        for half in (0, 1):
            for far in (0, 1):
                first_copy(pair, half, far).wait_send()
            second_copy(pair, half).wait_send()
        for mask in range(1, n_z):
            last_copy(pair, mask).wait_send()


def local(amplitudes, integrals, slot_tile):
    n_slab = lax.axis_size("slab")
    n_blk = lax.axis_size("blk")
    n_out, slot_dev, tile_len = amplitudes.shape[1:4]
    v_width = integrals.shape[-1]
    blocks = (v_width + tile_len - 1) // tile_len
    padded = blocks * tile_len
    row_part = tile_len // n_slab
    n_z = n_blk // 2
    half_z = n_z // 2
    assert n_slab == 4 and n_out == 3 and n_blk & (n_blk - 1) == 0 and n_blk >= 4
    bf16, f32 = amplitudes.dtype, jnp.float32
    piece = (slot_dev, row_part, tile_len)
    dma = pltpu.SemaphoreType.DMA
    n_slots = slot_tile.shape[0]
    slot_ids = jnp.arange(n_slots, dtype=jnp.int32)
    tile_ids = jnp.arange(blocks * blocks, dtype=jnp.int32)
    slot_of = jnp.sum(jnp.where(slot_tile[None] == tile_ids[:, None], slot_ids[None], 0), axis=1)
    come_from = jnp.stack([slot_of // slot_dev, slot_of % slot_dev])
    used = slot_tile >= 0
    safe = jnp.maximum(slot_tile, 0)
    tile_at = jnp.stack([safe // blocks, safe % blocks, used.astype(jnp.int32)])
    dims = (n_slab, n_blk, blocks, v_width, slot_dev, tile_len)
    return pl.pallas_call(
        functools.partial(cycle_kernel, dims),
        out_shape=jax.ShapeDtypeStruct((n_out,) + piece, f32),
        in_specs=[
            pl.BlockSpec(memory_space=pltpu.SMEM),
            pl.BlockSpec(memory_space=pltpu.SMEM),
            pl.BlockSpec(memory_space=pl.ANY),
            pl.BlockSpec(memory_space=pl.ANY),
        ],
        out_specs=pl.BlockSpec(memory_space=pltpu.VMEM),
        scratch_shapes=[pltpu.VMEM((n_blk, slot_dev, tile_len, tile_len), bf16)] * 3
        + [pltpu.VMEM((padded, padded), bf16)] * 3
        + [
            pltpu.VMEM((2, row_chunk(v_width), v_width), bf16),
            pltpu.VMEM((3, padded, padded), bf16),
            pltpu.VMEM((blocks, blocks, tile_len, tile_len), f32),
            pltpu.VMEM((blocks, blocks, tile_len, tile_len), f32),
            pltpu.VMEM((2, n_slab, n_z) + piece, f32),
            pltpu.VMEM((3, n_slab, n_z) + piece, f32),
            pltpu.VMEM((3, 2, 2, half_z) + piece, f32),
            pltpu.VMEM((3, 2, half_z) + piece, f32),
            pltpu.VMEM((3, n_z) + piece, f32),
            dma((2,)),
            dma((3,)),
            dma((3, n_blk)),
            dma((3, n_blk)),
            dma((3, 4)),
            dma((3, 4)),
            dma((3, 2, 2)),
            dma((3, 2, 2)),
            dma((3, 2)),
            dma((3, 2)),
            dma((3, n_z)),
            dma((3, n_z)),
        ],
        compiler_params=pltpu.CompilerParams(
            collective_id=0, has_side_effects=True, vmem_limit_bytes=67043328
        ),
        name="cycle",
    )(come_from, tile_at, amplitudes, integrals)


def solution(mesh):
    return jax.shard_map(
        local,
        mesh=mesh,
        in_specs=(P("slab", None, "blk", None, None), P(("slab", "blk"), None, None, None), P()),
        out_specs=P(None, "blk", "slab", None),
        check_vma=False,
    )
```

```python
import functools

import jax
import jax.numpy as jnp
from jax import lax
from jax.experimental import pallas as pl
from jax.experimental.pallas import tpu as pltpu
from jax.sharding import PartitionSpec as P

MESH = pl.DeviceIdType.MESH


def flip(index, mask):
    out = index
    bit = 1
    while bit <= mask:
        if mask & bit:
            out = out + bit * (1 - 2 * ((index // bit) % 2))
        bit *= 2
    return out


def row_chunk(rows):
    return max(size for size in range(16, 257, 16) if rows % size == 0)


def cycle_kernel(
    dims,
    of_ref, slot_ref, amp_ref, int_ref, out_ref,
    packed0, packed1, packed2, full0, full1, full2, landing, weights, acc_a, acc_b,
    outgoing, mates, first_in, second_in, last_in,
    load_sem, local_sem, amp_send, amp_recv, mate_send, mate_recv,
    first_send, first_recv, second_send, second_recv, last_send, last_recv,
):
    n_slab, n_blk, blocks, v_width, slot_dev, tile_len = dims
    n_z = n_blk // 2
    half_z = n_z // 2
    padded = blocks * tile_len
    row_part = tile_len // n_slab
    n_slots = n_blk * slot_dev
    packed = (packed0, packed1, packed2)
    fulls = (full0, full1, full2)
    slab = lax.axis_index("slab")
    blk = lax.axis_index("blk")
    core = blk % 2
    z_at = blk // 2

    barrier = pltpu.get_barrier_semaphore()
    for mask in range(1, n_blk):
        pl.semaphore_signal(barrier, inc=1, device_id={"blk": flip(blk, mask)}, device_id_type=MESH)
    for mask in (1, 2):
        pl.semaphore_signal(barrier, inc=1, device_id={"slab": flip(slab, mask)}, device_id_type=MESH)
    pl.semaphore_wait(barrier, n_blk + 1)

    def amp_copy(which, mask):
        target = flip(blk, mask)
        return pltpu.make_async_remote_copy(
            src_ref=amp_ref.at[target, which],
            dst_ref=packed[which].at[blk],
            send_sem=amp_send.at[which, mask],
            recv_sem=amp_recv.at[which, mask],
            device_id={"blk": target},
            device_id_type=MESH,
        )

    def own_copy(which):
        return pltpu.make_async_copy(amp_ref.at[blk, which], packed[which].at[blk], local_sem.at[which])

    order = tuple(reversed(range(1, n_blk)))
    for which in range(3):
        if which < 2:
            for mask in order:
                amp_copy(which, mask).start()
        own_copy(which).start()

    chunk = landing.shape[1]
    n_chunk = v_width // chunk
    pad = padded - v_width

    def int_copy(number):
        which, at = divmod(number, n_chunk)
        return pltpu.make_async_copy(
            int_ref.at[0, which, pl.ds(at * chunk, chunk)], landing.at[number % 2], load_sem.at[number % 2]
        )

    int_copy(0).start()
    for number in range(3 * n_chunk):
        which, at = divmod(number, n_chunk)
        if number + 1 < 3 * n_chunk:
            int_copy(number + 1).start()
        int_copy(number).wait()
        weights[which, pl.ds(at * chunk, chunk), pl.ds(0, v_width)] = landing[number % 2]
    if pad:
        for which in range(3):
            weights[which, :, pl.ds(v_width, pad)] = jnp.zeros((padded, pad), weights.dtype)
            weights[which, pl.ds(v_width, pad), :] = jnp.zeros((pad, padded), weights.dtype)

    gate = n_blk // 2
    amp_copy(1, gate).wait_recv()
    for mask in order:
        amp_copy(2, mask).start()

    row_ids = lax.broadcasted_iota(jnp.int32, (tile_len, tile_len), 0)
    col_ids = lax.broadcasted_iota(jnp.int32, (tile_len, tile_len), 1)

    def put_tile(which, x, y):
        at = x * blocks + y
        rows = pl.ds(pl.multiple_of(x * tile_len, tile_len), tile_len)
        cols = pl.ds(pl.multiple_of(y * tile_len, tile_len), tile_len)
        keep = jnp.logical_and(row_ids + x * tile_len < col_ids + y * tile_len, col_ids + y * tile_len < v_width)
        raw = packed[which][lax.div(of_ref[at], slot_dev), lax.rem(of_ref[at], slot_dev)]
        tile = jnp.where(keep, raw.astype(jnp.float32), 0.0)
        mirror = tile.T
        same = jnp.where(x == y, 1.0, 0.0)
        fulls[which][rows, cols] = (tile - same * mirror).astype(raw.dtype)
        fulls[which][cols, rows] = (same * tile - mirror).astype(raw.dtype)

    def build(which):
        for mask in range(1, n_blk):
            if (which, mask) != (1, gate):
                amp_copy(which, mask).wait_recv()
        own_copy(which).wait()
        if blocks % 2:
            for x in range(blocks):
                for y in range(x, blocks):
                    put_tile(which, x, y)
            return

        def fold(i, carry):
            for j in range(blocks + 1):
                upper = j < blocks - i
                x = jnp.where(upper, i, blocks - 1 - i)
                y = jnp.where(upper, i + j, j - 1)
                put_tile(which, x, y)
            return carry

        lax.fori_loop(0, blocks // 2, fold, 0)

    width = 2 * tile_len if padded % (2 * tile_len) == 0 else tile_len

    per_step = width // tile_len

    def product(left, right, cols):
        return jnp.dot(fulls[left][...], weights[right, :, cols], preferred_element_type=jnp.float32)

    def by_columns(acc, fresh, terms):
        def step(number, carry):
            cols = pl.ds(pl.multiple_of(number * width, width), width)
            total = None
            for sign, left, right in terms:
                term = product(left, right, cols)
                total = (term if sign > 0 else -term) if total is None else total + term if sign > 0 else total - term
            for x in range(blocks):
                for part in range(per_step):
                    y = number * per_step + part
                    tile = total[x * tile_len : (x + 1) * tile_len, part * tile_len : (part + 1) * tile_len]
                    acc[x, y] = tile if fresh else acc[x, y] + tile
            return carry

        lax.fori_loop(0, padded // width, step, 0)

    def pack(acc):
        def owner_tiles(owner, carry):
            for place in range(slot_dev):
                slot = owner * slot_dev + place
                tile_id = jnp.maximum(slot_ref[slot], 0)
                used = jnp.minimum(slot_ref[slot], 0) + 1
                first, second = lax.div(tile_id, blocks), lax.rem(tile_id, blocks)
                tile = (acc[first, second] - acc[second, first].T) * used.astype(jnp.float32)
                for part in range(n_slab):
                    outgoing[owner % 2, part, owner // 2, place] = tile[part * row_part : (part + 1) * row_part]
            return carry

        lax.fori_loop(0, n_blk, owner_tiles, 0)

    def mate_copy(pair, mask):
        part = flip(slab, mask)
        return pltpu.make_async_remote_copy(
            src_ref=outgoing.at[1 - core, part],
            dst_ref=mates.at[pair, part],
            send_sem=mate_send.at[pair, mask],
            recv_sem=mate_recv.at[pair, mask],
            device_id={"blk": flip(blk, 1)},
            device_id_type=MESH,
        )

    halves = (pl.ds(0, half_z), pl.ds(half_z, n_z - half_z))

    def first_copy(pair, half, far):
        mine, other = (1, 2) if half == 0 else (2, 1)
        part = flip(slab, 3 if far else mine)
        return pltpu.make_async_remote_copy(
            src_ref=mates.at[pair, part, halves[half]],
            dst_ref=first_in.at[pair, half, far],
            send_sem=first_send.at[pair, half, far],
            recv_sem=first_recv.at[pair, half, far],
            device_id={"slab": flip(slab, mine)},
            device_id_type=MESH,
        )

    def second_copy(pair, half):
        other = 2 if half == 0 else 1
        return pltpu.make_async_remote_copy(
            src_ref=mates.at[pair, flip(slab, other), halves[half]],
            dst_ref=second_in.at[pair, half],
            send_sem=second_send.at[pair, half],
            recv_sem=second_recv.at[pair, half],
            device_id={"slab": flip(slab, other)},
            device_id_type=MESH,
        )

    def last_copy(pair, mask):
        target = flip(z_at, mask)
        return pltpu.make_async_remote_copy(
            src_ref=mates.at[pair, slab, target],
            dst_ref=last_in.at[pair, mask],
            send_sem=last_send.at[pair, mask],
            recv_sem=last_recv.at[pair, mask],
            device_id={"blk": target * 2 + core},
            device_id_type=MESH,
        )

    def mates_start(pair):
        for mask in (3, 1, 2, 0):
            mate_copy(pair, mask).start()

    def mates_finish(pair):
        for mask in (3, 1, 2, 0):
            mate_copy(pair, mask).wait_recv()
            part = flip(slab, mask)
            mates[pair, part] = mates[pair, part] + outgoing[core, part]
            if mask == 3:
                first_copy(pair, 0, 1).start()
                first_copy(pair, 1, 1).start()
            if mask == 1:
                first_copy(pair, 0, 0).start()
            if mask == 2:
                first_copy(pair, 1, 0).start()
        for mask in (3, 1, 2, 0):
            mate_copy(pair, mask).wait_send()

    def first_finish(pair):
        for half in (0, 1):
            part = flip(slab, 2 if half == 0 else 1)
            first_copy(pair, half, 1).wait_recv()
            mates[pair, part, halves[half]] = mates[pair, part, halves[half]] + first_in[pair, half, 1]
            second_copy(pair, half).start()

    def second_finish(pair):
        for half in (0, 1):
            first_copy(pair, half, 0).wait_recv()
            second_copy(pair, half).wait_recv()
            mates[pair, slab, halves[half]] = (
                mates[pair, slab, halves[half]] + first_in[pair, half, 0] + second_in[pair, half]
            )

    def last_start(pair):
        for mask in reversed(range(1, n_z)):
            last_copy(pair, mask).start()

    def last_finish(pair):
        total = mates[pair, slab, z_at]
        for mask in range(1, n_z):
            last_copy(pair, mask).wait_recv()
            total = total + last_in[pair, mask]
        out_ref[pair] = total

    pair01, pair02, pair12 = 0, 1, 2
    build(0)
    build(1)

    by_columns(acc_a, True, ((1, 0, 1), (-1, 1, 0)))
    pack(acc_a)
    mates_start(pair01)

    by_columns(acc_b, True, ((1, 0, 2),))
    mates_finish(pair01)

    by_columns(acc_a, True, ((1, 1, 2),))
    first_finish(pair01)
    second_finish(pair01)

    build(2)
    last_start(pair01)

    by_columns(acc_b, False, ((-1, 2, 0),))
    pack(acc_b)
    mates_start(pair02)

    by_columns(acc_a, False, ((-1, 2, 1),))
    mates_finish(pair02)
    pack(acc_a)
    mates_start(pair12)
    first_finish(pair02)
    mates_finish(pair12)
    second_finish(pair02)
    last_start(pair02)
    first_finish(pair12)
    last_finish(pair01)
    second_finish(pair12)
    last_start(pair12)
    last_finish(pair02)
    last_finish(pair12)

    for which in range(3):
        for mask in range(1, n_blk):
            amp_copy(which, mask).wait_send()
    for pair in (pair01, pair02, pair12):
        for half in (0, 1):
            for far in (0, 1):
                first_copy(pair, half, far).wait_send()
            second_copy(pair, half).wait_send()
        for mask in range(1, n_z):
            last_copy(pair, mask).wait_send()


def local(amplitudes, integrals, slot_tile):
    n_slab = lax.axis_size("slab")
    n_blk = lax.axis_size("blk")
    n_out, slot_dev, tile_len = amplitudes.shape[1:4]
    v_width = integrals.shape[-1]
    blocks = (v_width + tile_len - 1) // tile_len
    padded = blocks * tile_len
    row_part = tile_len // n_slab
    n_z = n_blk // 2
    half_z = n_z // 2
    assert n_slab == 4 and n_out == 3 and n_blk & (n_blk - 1) == 0 and n_blk >= 4
    bf16, f32 = amplitudes.dtype, jnp.float32
    piece = (slot_dev, row_part, tile_len)
    dma = pltpu.SemaphoreType.DMA
    n_slots = slot_tile.shape[0]
    slot_ids = jnp.arange(n_slots, dtype=jnp.int32)
    tile_ids = jnp.arange(blocks * blocks, dtype=jnp.int32)
    slot_of = jnp.sum(jnp.where(slot_tile[None] == tile_ids[:, None], slot_ids[None], 0), axis=1)
    dims = (n_slab, n_blk, blocks, v_width, slot_dev, tile_len)
    return pl.pallas_call(
        functools.partial(cycle_kernel, dims),
        out_shape=jax.ShapeDtypeStruct((n_out,) + piece, f32),
        in_specs=[
            pl.BlockSpec(memory_space=pltpu.SMEM),
            pl.BlockSpec(memory_space=pltpu.SMEM),
            pl.BlockSpec(memory_space=pl.ANY),
            pl.BlockSpec(memory_space=pl.ANY),
        ],
        out_specs=pl.BlockSpec(memory_space=pltpu.VMEM),
        scratch_shapes=[pltpu.VMEM((n_blk, slot_dev, tile_len, tile_len), bf16)] * 3
        + [pltpu.VMEM((padded, padded), bf16)] * 3
        + [
            pltpu.VMEM((2, row_chunk(v_width), v_width), bf16),
            pltpu.VMEM((3, padded, padded), bf16),
            pltpu.VMEM((blocks, blocks, tile_len, tile_len), f32),
            pltpu.VMEM((blocks, blocks, tile_len, tile_len), f32),
            pltpu.VMEM((2, n_slab, n_z) + piece, f32),
            pltpu.VMEM((3, n_slab, n_z) + piece, f32),
            pltpu.VMEM((3, 2, 2, half_z) + piece, f32),
            pltpu.VMEM((3, 2, half_z) + piece, f32),
            pltpu.VMEM((3, n_z) + piece, f32),
            dma((2,)),
            dma((3,)),
            dma((3, n_blk)),
            dma((3, n_blk)),
            dma((3, 4)),
            dma((3, 4)),
            dma((3, 2, 2)),
            dma((3, 2, 2)),
            dma((3, 2)),
            dma((3, 2)),
            dma((3, n_z)),
            dma((3, n_z)),
        ],
        compiler_params=pltpu.CompilerParams(
            collective_id=0, has_side_effects=True, vmem_limit_bytes=67043328
        ),
        name="cycle",
    )(slot_of, slot_tile, amplitudes, integrals)


def solution(mesh):
    return jax.shard_map(
        local,
        mesh=mesh,
        in_specs=(P("slab", None, "blk", None, None), P(("slab", "blk"), None, None, None), P()),
        out_specs=P(None, "blk", "slab", None),
        check_vma=False,
    )
```

```python
import functools

import jax
import jax.numpy as jnp
from jax import lax
from jax.experimental import pallas as pl
from jax.experimental.pallas import tpu as pltpu
from jax.sharding import PartitionSpec as P

MESH = pl.DeviceIdType.MESH
PARTS = (3, 1, 2, 0)
EARLY = 2


def flip(index, mask):
    out = index
    bit = 1
    while bit <= mask:
        if mask & bit:
            out = out + bit * (1 - 2 * ((index // bit) % 2))
        bit *= 2
    return out


def plain_places(slot_dev):
    return max(1, slot_dev * 5 // 7), max(1, slot_dev * 5 // 7)


def row_chunk(rows):
    return max(size for size in range(16, 257, 16) if rows % size == 0)


def cycle_kernel(
    dims,
    of_ref, slot_ref, amp_ref, int_ref, out_ref,
    packed0, packed1, packed2, full0, full1, full2, landing, weights, acc_a, acc_b,
    outgoing, mates, low_in, first_in, second_in, last_in,
    load_sem, local_sem, amp_send, amp_recv, mate_send, mate_recv, low_send, low_recv,
    first_send, first_recv, second_send, second_recv, last_send, last_recv,
):
    n_slab, n_blk, blocks, v_width, slot_dev, tile_len = dims
    n_z = n_blk // 2
    padded = blocks * tile_len
    cut = plain_places(slot_dev)
    jobs = (
        (0, pl.ds(0, slot_dev), False),
        (1, pl.ds(0, cut[0]), False),
        (1, pl.ds(cut[0], slot_dev - cut[0]), True),
        (2, pl.ds(0, cut[1]), False),
        (2, pl.ds(cut[1], slot_dev - cut[1]), True),
    )
    whole01, plain02, low02, plain12, low12 = range(5)
    row_part = tile_len // n_slab
    n_slots = n_blk * slot_dev
    packed = (packed0, packed1, packed2)
    fulls = (full0, full1, full2)
    slab = lax.axis_index("slab")
    blk = lax.axis_index("blk")
    core = blk % 2
    z_at = blk // 2

    barrier = pltpu.get_barrier_semaphore()
    for mask in range(1, n_blk):
        pl.semaphore_signal(barrier, inc=1, device_id={"blk": flip(blk, mask)}, device_id_type=MESH)
    for mask in (1, 2):
        pl.semaphore_signal(barrier, inc=1, device_id={"slab": flip(slab, mask)}, device_id_type=MESH)
    pl.semaphore_wait(barrier, n_blk + 1)

    def amp_copy(which, mask):
        target = flip(blk, mask)
        return pltpu.make_async_remote_copy(
            src_ref=amp_ref.at[target, which],
            dst_ref=packed[which].at[blk],
            send_sem=amp_send.at[which, mask],
            recv_sem=amp_recv.at[which, mask],
            device_id={"blk": target},
            device_id_type=MESH,
        )

    def own_copy(which):
        return pltpu.make_async_copy(amp_ref.at[blk, which], packed[which].at[blk], local_sem.at[which])

    order = tuple(reversed(range(1, n_blk)))
    for which in range(3):
        if which < 2:
            for mask in order:
                amp_copy(which, mask).start()
        own_copy(which).start()

    chunk = landing.shape[1]
    n_chunk = v_width // chunk
    pad = padded - v_width

    def int_copy(number):
        which, at = divmod(number, n_chunk)
        return pltpu.make_async_copy(
            int_ref.at[0, which, pl.ds(at * chunk, chunk)], landing.at[number % 2], load_sem.at[number % 2]
        )

    int_copy(0).start()
    for number in range(3 * n_chunk):
        which, at = divmod(number, n_chunk)
        if number + 1 < 3 * n_chunk:
            int_copy(number + 1).start()
        int_copy(number).wait()
        weights[which, pl.ds(at * chunk, chunk), pl.ds(0, v_width)] = landing[number % 2]
    if pad:
        for which in range(3):
            weights[which, :, pl.ds(v_width, pad)] = jnp.zeros((padded, pad), weights.dtype)
            weights[which, pl.ds(v_width, pad), :] = jnp.zeros((pad, padded), weights.dtype)

    gate = n_blk // 2
    amp_copy(1, gate).wait_recv()
    for mask in order:
        amp_copy(2, mask).start()

    row_ids = lax.broadcasted_iota(jnp.int32, (tile_len, tile_len), 0)
    col_ids = lax.broadcasted_iota(jnp.int32, (tile_len, tile_len), 1)

    def put_tile(which, x, y):
        at = x * blocks + y
        rows = pl.ds(pl.multiple_of(x * tile_len, tile_len), tile_len)
        cols = pl.ds(pl.multiple_of(y * tile_len, tile_len), tile_len)
        keep = jnp.logical_and(row_ids + x * tile_len < col_ids + y * tile_len, col_ids + y * tile_len < v_width)
        raw = packed[which][lax.div(of_ref[at], slot_dev), lax.rem(of_ref[at], slot_dev)]
        tile = jnp.where(keep, raw.astype(jnp.float32), 0.0)
        mirror = tile.T
        same = jnp.where(x == y, 1.0, 0.0)
        fulls[which][rows, cols] = (tile - same * mirror).astype(raw.dtype)
        fulls[which][cols, rows] = (same * tile - mirror).astype(raw.dtype)

    def arrive(which):
        for mask in range(1, n_blk):
            if (which, mask) != (1, gate):
                amp_copy(which, mask).wait_recv()
        own_copy(which).wait()

    def build(which):
        if blocks % 2:
            for x in range(blocks):
                for y in range(x, blocks):
                    put_tile(which, x, y)
            return

        def fold(i, carry):
            for j in range(blocks + 1):
                upper = j < blocks - i
                x = jnp.where(upper, i, blocks - 1 - i)
                y = jnp.where(upper, i + j, j - 1)
                put_tile(which, x, y)
            return carry

        lax.fori_loop(0, blocks // 2, fold, 0)

    width = 2 * tile_len if padded % (2 * tile_len) == 0 else tile_len

    per_step = width // tile_len

    def product(left, right, cols):
        return jnp.dot(fulls[left][...], weights[right, :, cols], preferred_element_type=jnp.float32)

    def by_columns(acc, fresh, terms, start=0, stop=padded // width):
        def step(number, carry):
            cols = pl.ds(pl.multiple_of(number * width, width), width)
            total = None
            for sign, left, right in terms:
                term = product(left, right, cols)
                total = (term if sign > 0 else -term) if total is None else total + term if sign > 0 else total - term
            for x in range(blocks):
                for part in range(per_step):
                    y = number * per_step + part
                    tile = total[x * tile_len : (x + 1) * tile_len, part * tile_len : (part + 1) * tile_len]
                    acc[x, y] = tile if fresh else acc[x, y] + tile
            return carry

        lax.fori_loop(start, stop, step, 0)

    def pack(acc, pair):
        def tiles_of(core_at):
            def owner_tiles(z, carry):
                for place in range(slot_dev):
                    slot = (z * 2 + core_at) * slot_dev + place
                    tile_id = jnp.maximum(slot_ref[slot], 0)
                    used = jnp.minimum(slot_ref[slot], 0) + 1
                    first, second = lax.div(tile_id, blocks), lax.rem(tile_id, blocks)
                    tile = (acc[first, second] - acc[second, first].T) * used.astype(jnp.float32)
                    for part in range(n_slab):
                        rows = tile[part * row_part : (part + 1) * row_part]
                        outgoing[core_at, part // 2, part % 2, z // 2, z % 2, place] = rows
                return carry

            lax.fori_loop(0, n_z, owner_tiles, 0)

        tiles_of(1 - core)
        for mask in PARTS:
            mate_copy(pair, mask).start()
        tiles_of(core)

    s_y, s_x = slab // 2, slab % 2
    z_hi, z_lo = z_at // 2, z_at % 2
    n_hi = n_z // 2
    halves = (pl.ds(0, n_hi // 2), pl.ds(n_hi // 2, n_hi - n_hi // 2))

    def part_of(mask):
        return (1 - s_y if mask & 2 else s_y), (1 - s_x if mask & 1 else s_x)

    def mate_copy(pair, mask):
        p_y, p_x = part_of(mask)
        return pltpu.make_async_remote_copy(
            src_ref=outgoing.at[1 - core, p_y, p_x],
            dst_ref=mates.at[pair, p_y, p_x],
            send_sem=mate_send.at[pair, mask],
            recv_sem=mate_recv.at[pair, mask],
            device_id={"blk": flip(blk, 1)},
            device_id_type=MESH,
        )

    def low_copy(job, mask):
        pair, places, _ = jobs[job]
        p_y, p_x = part_of(mask)
        return pltpu.make_async_remote_copy(
            src_ref=mates.at[pair, p_y, p_x, :, 1 - z_lo, places],
            dst_ref=low_in.at[pair, p_y, p_x, :, places],
            send_sem=low_send.at[job, mask],
            recv_sem=low_recv.at[job, mask],
            device_id={"blk": flip(blk, 2)},
            device_id_type=MESH,
        )

    def z_range(job):
        return z_lo if jobs[job][2] else slice(None)

    def first_copy(job, half, far):
        pair, places, _ = jobs[job]
        mine = 1 if half == 0 else 2
        p_y, p_x = part_of(3 if far else mine)
        return pltpu.make_async_remote_copy(
            src_ref=mates.at[pair, p_y, p_x, halves[half], z_range(job), places],
            dst_ref=first_in.at[pair, half, far, :, z_range(job), places],
            send_sem=first_send.at[job, half, far],
            recv_sem=first_recv.at[job, half, far],
            device_id={"slab": flip(slab, mine)},
            device_id_type=MESH,
        )

    def second_copy(job, half):
        pair, places, _ = jobs[job]
        other = 2 if half == 0 else 1
        p_y, p_x = part_of(other)
        return pltpu.make_async_remote_copy(
            src_ref=mates.at[pair, p_y, p_x, halves[half], z_range(job), places],
            dst_ref=second_in.at[pair, half, :, z_range(job), places],
            send_sem=second_send.at[job, half],
            recv_sem=second_recv.at[job, half],
            device_id={"slab": flip(slab, other)},
            device_id_type=MESH,
        )

    def last_masks(job):
        return [mask for mask in reversed(range(1, n_z)) if not (jobs[job][2] and mask % 2)]

    def last_copy(job, mask):
        pair, places, _ = jobs[job]
        target = flip(z_at, mask)
        return pltpu.make_async_remote_copy(
            src_ref=mates.at[pair, s_y, s_x, target // 2, target % 2, places],
            dst_ref=last_in.at[pair, mask, places],
            send_sem=last_send.at[job, mask],
            recv_sem=last_recv.at[job, mask],
            device_id={"blk": target * 2 + core},
            device_id_type=MESH,
        )

    def first_start(job, mask):
        if mask == 3:
            first_copy(job, 0, 1).start()
            first_copy(job, 1, 1).start()
        elif mask:
            first_copy(job, mask - 1, 0).start()

    def mates_finish(pair):
        for mask in PARTS:
            mate_copy(pair, mask).wait_recv()
            p_y, p_x = part_of(mask)
            mates[pair, p_y, p_x] = mates[pair, p_y, p_x] + outgoing[core, p_y, p_x]
            for job, (owner, _, low) in enumerate(jobs):
                if owner == pair and low:
                    low_copy(job, mask).start()
                elif owner == pair:
                    first_start(job, mask)
        for mask in PARTS:
            mate_copy(pair, mask).wait_send()

    def low_finish(job):
        pair, places, _ = jobs[job]
        for mask in PARTS:
            low_copy(job, mask).wait_recv()
            p_y, p_x = part_of(mask)
            mates[pair, p_y, p_x, :, z_lo, places] = (
                mates[pair, p_y, p_x, :, z_lo, places] + low_in[pair, p_y, p_x, :, places]
            )
            first_start(job, mask)

    def first_finish(job):
        pair, places, _ = jobs[job]
        for half in (0, 1):
            at = (pair, *part_of(2 if half == 0 else 1), halves[half], z_range(job), places)
            first_copy(job, half, 1).wait_recv()
            mates[at] = mates[at] + first_in[pair, half, 1, :, z_range(job), places]
            second_copy(job, half).start()

    def second_finish(job):
        pair, places, _ = jobs[job]
        for half in (0, 1):
            at = (pair, s_y, s_x, halves[half], z_range(job), places)
            first_copy(job, half, 0).wait_recv()
            second_copy(job, half).wait_recv()
            mates[at] = (
                mates[at]
                + first_in[pair, half, 0, :, z_range(job), places]
                + second_in[pair, half, :, z_range(job), places]
            )

    def last_start(job):
        for mask in last_masks(job):
            last_copy(job, mask).start()

    def last_finish(job):
        pair, places, _ = jobs[job]
        total = mates[pair, s_y, s_x, z_hi, z_lo, places]
        for mask in last_masks(job):
            last_copy(job, mask).wait_recv()
            total = total + last_in[pair, mask, places]
        out_ref[pair, places] = total

    pair01, pair02, pair12 = 0, 1, 2
    arrive(0)
    build(0)
    arrive(1)
    build(1)
    by_columns(acc_a, True, ((1, 0, 1), (-1, 1, 0)))
    pack(acc_a, pair01)
    by_columns(acc_b, True, ((1, 0, 2),))
    mates_finish(pair01)
    by_columns(acc_a, True, ((1, 1, 2),))
    first_finish(whole01)
    second_finish(whole01)

    arrive(2)
    last_start(whole01)
    build(2)
    by_columns(acc_b, False, ((-1, 2, 0),))
    pack(acc_b, pair02)
    by_columns(acc_a, False, ((-1, 2, 1),), 0, EARLY)
    mates_finish(pair02)
    by_columns(acc_a, False, ((-1, 2, 1),), EARLY)
    first_finish(plain02)
    pack(acc_a, pair12)
    low_finish(low02)
    mates_finish(pair12)
    second_finish(plain02)
    last_start(plain02)
    first_finish(low02)
    first_finish(plain12)
    second_finish(low02)
    last_start(low02)
    low_finish(low12)
    first_finish(low12)
    second_finish(plain12)
    last_start(plain12)
    second_finish(low12)
    last_start(low12)
    for job in range(len(jobs)):
        last_finish(job)

    for mask in order:
        amp_copy(0, mask).wait_send()
        amp_copy(1, mask).wait_send()
        amp_copy(2, mask).wait_send()
    for job, (_, _, low) in enumerate(jobs):
        for mask in PARTS:
            if low:
                low_copy(job, mask).wait_send()
        for half in (0, 1):
            for far in (0, 1):
                first_copy(job, half, far).wait_send()
            second_copy(job, half).wait_send()
        for mask in last_masks(job):
            last_copy(job, mask).wait_send()


def local(amplitudes, integrals, slot_tile):
    n_slab = lax.axis_size("slab")
    n_blk = lax.axis_size("blk")
    n_out, slot_dev, tile_len = amplitudes.shape[1:4]
    v_width = integrals.shape[-1]
    blocks = (v_width + tile_len - 1) // tile_len
    padded = blocks * tile_len
    row_part = tile_len // n_slab
    n_z = n_blk // 2
    half_hi = n_z // 4
    n_jobs = 5
    assert n_slab == 4 and n_out == 3 and n_blk & (n_blk - 1) == 0 and n_blk >= 8 and slot_dev > 1
    bf16, f32 = amplitudes.dtype, jnp.float32
    piece = (slot_dev, row_part, tile_len)
    dma = pltpu.SemaphoreType.DMA
    n_slots = slot_tile.shape[0]
    slot_ids = jnp.arange(n_slots, dtype=jnp.int32)
    tile_ids = jnp.arange(blocks * blocks, dtype=jnp.int32)
    slot_of = jnp.sum(jnp.where(slot_tile[None] == tile_ids[:, None], slot_ids[None], 0), axis=1)
    dims = (n_slab, n_blk, blocks, v_width, slot_dev, tile_len)
    return pl.pallas_call(
        functools.partial(cycle_kernel, dims),
        out_shape=jax.ShapeDtypeStruct((n_out,) + piece, f32),
        in_specs=[
            pl.BlockSpec(memory_space=pltpu.SMEM),
            pl.BlockSpec(memory_space=pltpu.SMEM),
            pl.BlockSpec(memory_space=pl.ANY),
            pl.BlockSpec(memory_space=pl.ANY),
        ],
        out_specs=pl.BlockSpec(memory_space=pltpu.VMEM),
        scratch_shapes=[pltpu.VMEM((n_blk, slot_dev, tile_len, tile_len), bf16)] * 3
        + [pltpu.VMEM((padded, padded), bf16)] * 3
        + [
            pltpu.VMEM((2, row_chunk(v_width), v_width), bf16),
            pltpu.VMEM((3, padded, padded), bf16),
            pltpu.VMEM((blocks, blocks, tile_len, tile_len), f32),
            pltpu.VMEM((blocks, blocks, tile_len, tile_len), f32),
            pltpu.VMEM((2, 2, 2, n_z // 2, 2) + piece, f32),
            pltpu.VMEM((3, 2, 2, n_z // 2, 2) + piece, f32),
            pltpu.VMEM((3, 2, 2, n_z // 2) + piece, f32),
            pltpu.VMEM((3, 2, 2, half_hi, 2) + piece, f32),
            pltpu.VMEM((3, 2, half_hi, 2) + piece, f32),
            pltpu.VMEM((3, n_z) + piece, f32),
            dma((2,)),
            dma((3,)),
            dma((3, n_blk)),
            dma((3, n_blk)),
            dma((3, 4)),
            dma((3, 4)),
            dma((n_jobs, 4)),
            dma((n_jobs, 4)),
            dma((n_jobs, 2, 2)),
            dma((n_jobs, 2, 2)),
            dma((n_jobs, 2)),
            dma((n_jobs, 2)),
            dma((n_jobs, n_z)),
            dma((n_jobs, n_z)),
        ],
        compiler_params=pltpu.CompilerParams(
            collective_id=0, has_side_effects=True, vmem_limit_bytes=67043328
        ),
        name="cycle",
    )(slot_of, slot_tile, amplitudes, integrals)


def solution(mesh):
    return jax.shard_map(
        local,
        mesh=mesh,
        in_specs=(P("slab", None, "blk", None, None), P(("slab", "blk"), None, None, None), P()),
        out_specs=P(None, "blk", "slab", None),
        check_vma=False,
    )
```

```python
import functools

import jax
import jax.numpy as jnp
from jax import lax
from jax.experimental import pallas as pl
from jax.experimental.pallas import tpu as pltpu
from jax.sharding import PartitionSpec as P

MESH = pl.DeviceIdType.MESH
PARTS = (3, 1, 2, 0)
EARLY = 2


def flip(index, mask):
    out = index
    bit = 1
    while bit <= mask:
        if mask & bit:
            out = out + bit * (1 - 2 * ((index // bit) % 2))
        bit *= 2
    return out


def row_chunk(rows):
    return max(size for size in range(16, 257, 16) if rows % size == 0)


def cycle_kernel(
    dims,
    of_ref, slot_ref, amp_ref, int_ref, out_ref,
    packed0, packed1, packed2, full0, full1, full2, landing, weights, acc_a, acc_b,
    outgoing, mates, low_in, first_in, second_in, last_in,
    load_sem, local_sem, amp_send, amp_recv, mate_send, mate_recv, low_send, low_recv,
    first_send, first_recv, second_send, second_recv, last_send, last_recv,
):
    n_slab, n_blk, blocks, v_width, slot_dev, tile_len = dims
    n_z = n_blk // 2
    padded = blocks * tile_len
    c0, c1, c2 = (max(1, slot_dev * c // 7) for c in (4, 3, 5))
    jobs = (
        (0, pl.ds(0, slot_dev), False),
        (1, pl.ds(0, c0), False),
        (1, pl.ds(c0, slot_dev - c0), True),
        (2, pl.ds(0, c1), False),
        (2, pl.ds(c1, c2 - c1), False),
        (2, pl.ds(c2, slot_dev - c2), True),
    )
    whole01, plain02, low02, plain12, more12, low12 = range(6)
    row_part = tile_len // n_slab
    n_slots = n_blk * slot_dev
    packed = (packed0, packed1, packed2)
    fulls = (full0, full1, full2)
    slab = lax.axis_index("slab")
    blk = lax.axis_index("blk")
    core = blk % 2
    z_at = blk // 2

    barrier = pltpu.get_barrier_semaphore()
    for mask in range(1, n_blk):
        pl.semaphore_signal(barrier, inc=1, device_id={"blk": flip(blk, mask)}, device_id_type=MESH)
    for mask in (1, 2):
        pl.semaphore_signal(barrier, inc=1, device_id={"slab": flip(slab, mask)}, device_id_type=MESH)
    pl.semaphore_wait(barrier, n_blk + 1)

    def amp_copy(which, mask):
        target = flip(blk, mask)
        return pltpu.make_async_remote_copy(
            src_ref=amp_ref.at[target, which],
            dst_ref=packed[which].at[blk],
            send_sem=amp_send.at[which, mask],
            recv_sem=amp_recv.at[which, mask],
            device_id={"blk": target},
            device_id_type=MESH,
        )

    def own_copy(which):
        return pltpu.make_async_copy(amp_ref.at[blk, which], packed[which].at[blk], local_sem.at[which])

    order = tuple(reversed(range(1, n_blk)))
    for which in range(3):
        if which < 2:
            for mask in order:
                amp_copy(which, mask).start()
        own_copy(which).start()

    chunk = landing.shape[1]
    n_chunk = v_width // chunk
    pad = padded - v_width

    def int_copy(number):
        which, at = divmod(number, n_chunk)
        return pltpu.make_async_copy(
            int_ref.at[0, which, pl.ds(at * chunk, chunk)], landing.at[number % 2], load_sem.at[number % 2]
        )

    int_copy(0).start()
    for number in range(3 * n_chunk):
        which, at = divmod(number, n_chunk)
        if number + 1 < 3 * n_chunk:
            int_copy(number + 1).start()
        int_copy(number).wait()
        weights[which, pl.ds(at * chunk, chunk), pl.ds(0, v_width)] = landing[number % 2]
    if pad:
        for which in range(3):
            weights[which, :, pl.ds(v_width, pad)] = jnp.zeros((padded, pad), weights.dtype)
            weights[which, pl.ds(v_width, pad), :] = jnp.zeros((pad, padded), weights.dtype)

    gate = n_blk // 2
    amp_copy(1, gate).wait_recv()
    for mask in order:
        amp_copy(2, mask).start()

    row_ids = lax.broadcasted_iota(jnp.int32, (tile_len, tile_len), 0)
    col_ids = lax.broadcasted_iota(jnp.int32, (tile_len, tile_len), 1)

    def put_tile(which, x, y):
        at = x * blocks + y
        rows = pl.ds(pl.multiple_of(x * tile_len, tile_len), tile_len)
        cols = pl.ds(pl.multiple_of(y * tile_len, tile_len), tile_len)
        keep = jnp.logical_and(row_ids + x * tile_len < col_ids + y * tile_len, col_ids + y * tile_len < v_width)
        raw = packed[which][lax.div(of_ref[at], slot_dev), lax.rem(of_ref[at], slot_dev)]
        tile = jnp.where(keep, raw.astype(jnp.float32), 0.0)
        mirror = tile.T
        same = jnp.where(x == y, 1.0, 0.0)
        fulls[which][rows, cols] = (tile - same * mirror).astype(raw.dtype)
        fulls[which][cols, rows] = (same * tile - mirror).astype(raw.dtype)

    def arrive(which):
        for mask in range(1, n_blk):
            if (which, mask) != (1, gate):
                amp_copy(which, mask).wait_recv()
        own_copy(which).wait()

    def build(which):
        if blocks % 2:
            for x in range(blocks):
                for y in range(x, blocks):
                    put_tile(which, x, y)
            return

        def fold(i, carry):
            for j in range(blocks + 1):
                upper = j < blocks - i
                x = jnp.where(upper, i, blocks - 1 - i)
                y = jnp.where(upper, i + j, j - 1)
                put_tile(which, x, y)
            return carry

        lax.fori_loop(0, blocks // 2, fold, 0)

    width = 2 * tile_len if padded % (2 * tile_len) == 0 else tile_len

    per_step = width // tile_len

    def product(left, right, cols):
        return jnp.dot(fulls[left][...], weights[right, :, cols], preferred_element_type=jnp.float32)

    def by_columns(acc, fresh, terms, start=0, stop=padded // width):
        def step(number, carry):
            cols = pl.ds(pl.multiple_of(number * width, width), width)
            total = None
            for sign, left, right in terms:
                term = product(left, right, cols)
                total = (term if sign > 0 else -term) if total is None else total + term if sign > 0 else total - term
            for x in range(blocks):
                for part in range(per_step):
                    y = number * per_step + part
                    tile = total[x * tile_len : (x + 1) * tile_len, part * tile_len : (part + 1) * tile_len]
                    acc[x, y] = tile if fresh else acc[x, y] + tile
            return carry

        lax.fori_loop(start, stop, step, 0)

    def pack(acc, pair):
        def tiles_of(core_at):
            def owner_tiles(z, carry):
                for place in range(slot_dev):
                    slot = (z * 2 + core_at) * slot_dev + place
                    tile_id = jnp.maximum(slot_ref[slot], 0)
                    used = jnp.minimum(slot_ref[slot], 0) + 1
                    first, second = lax.div(tile_id, blocks), lax.rem(tile_id, blocks)
                    tile = (acc[first, second] - acc[second, first].T) * used.astype(jnp.float32)
                    for part in range(n_slab):
                        rows = tile[part * row_part : (part + 1) * row_part]
                        outgoing[core_at, part // 2, part % 2, z // 2, z % 2, place] = rows
                return carry

            lax.fori_loop(0, n_z, owner_tiles, 0)

        tiles_of(1 - core)
        for mask in PARTS:
            mate_copy(pair, mask).start()
        tiles_of(core)

    s_y, s_x = slab // 2, slab % 2
    z_hi, z_lo = z_at // 2, z_at % 2
    n_hi = n_z // 2
    halves = (pl.ds(0, n_hi // 2), pl.ds(n_hi // 2, n_hi - n_hi // 2))

    def part_of(mask):
        return (1 - s_y if mask & 2 else s_y), (1 - s_x if mask & 1 else s_x)

    def mate_copy(pair, mask):
        p_y, p_x = part_of(mask)
        return pltpu.make_async_remote_copy(
            src_ref=outgoing.at[1 - core, p_y, p_x],
            dst_ref=mates.at[pair, p_y, p_x],
            send_sem=mate_send.at[pair, mask],
            recv_sem=mate_recv.at[pair, mask],
            device_id={"blk": flip(blk, 1)},
            device_id_type=MESH,
        )

    def held(job):
        return jobs[job][1].size > 0

    def low_copy(job, mask):
        pair, places, _ = jobs[job]
        p_y, p_x = part_of(mask)
        return pltpu.make_async_remote_copy(
            src_ref=mates.at[pair, p_y, p_x, :, 1 - z_lo, places],
            dst_ref=low_in.at[pair, p_y, p_x, :, places],
            send_sem=low_send.at[job, mask],
            recv_sem=low_recv.at[job, mask],
            device_id={"blk": flip(blk, 2)},
            device_id_type=MESH,
        )

    def z_range(job):
        return z_lo if jobs[job][2] else slice(None)

    def first_copy(job, half, far):
        pair, places, _ = jobs[job]
        mine = 1 if half == 0 else 2
        p_y, p_x = part_of(3 if far else mine)
        return pltpu.make_async_remote_copy(
            src_ref=mates.at[pair, p_y, p_x, halves[half], z_range(job), places],
            dst_ref=first_in.at[pair, half, far, :, z_range(job), places],
            send_sem=first_send.at[job, half, far],
            recv_sem=first_recv.at[job, half, far],
            device_id={"slab": flip(slab, mine)},
            device_id_type=MESH,
        )

    def second_copy(job, half):
        pair, places, _ = jobs[job]
        other = 2 if half == 0 else 1
        p_y, p_x = part_of(other)
        return pltpu.make_async_remote_copy(
            src_ref=mates.at[pair, p_y, p_x, halves[half], z_range(job), places],
            dst_ref=second_in.at[pair, half, :, z_range(job), places],
            send_sem=second_send.at[job, half],
            recv_sem=second_recv.at[job, half],
            device_id={"slab": flip(slab, other)},
            device_id_type=MESH,
        )

    def last_masks(job):
        return [mask for mask in reversed(range(1, n_z)) if not (jobs[job][2] and mask % 2)]

    def last_copy(job, mask):
        pair, places, _ = jobs[job]
        target = flip(z_at, mask)
        return pltpu.make_async_remote_copy(
            src_ref=mates.at[pair, s_y, s_x, target // 2, target % 2, places],
            dst_ref=last_in.at[pair, mask, places],
            send_sem=last_send.at[job, mask],
            recv_sem=last_recv.at[job, mask],
            device_id={"blk": target * 2 + core},
            device_id_type=MESH,
        )

    def first_start(job, mask):
        if not held(job):
            return
        if mask == 3:
            first_copy(job, 0, 1).start()
            first_copy(job, 1, 1).start()
        elif mask:
            first_copy(job, mask - 1, 0).start()

    def mates_finish(pair):
        for mask in PARTS:
            mate_copy(pair, mask).wait_recv()
            p_y, p_x = part_of(mask)
            mates[pair, p_y, p_x] = mates[pair, p_y, p_x] + outgoing[core, p_y, p_x]
            for job, (owner, _, low) in enumerate(jobs):
                if owner == pair and low:
                    low_copy(job, mask).start()
                elif owner == pair and job != more12:
                    first_start(job, mask)
        for mask in PARTS:
            mate_copy(pair, mask).wait_send()

    def low_finish(job):
        if not held(job):
            return
        pair, places, _ = jobs[job]
        for mask in PARTS:
            low_copy(job, mask).wait_recv()
            p_y, p_x = part_of(mask)
            mates[pair, p_y, p_x, :, z_lo, places] = (
                mates[pair, p_y, p_x, :, z_lo, places] + low_in[pair, p_y, p_x, :, places]
            )
            first_start(job, mask)

    def first_finish(job):
        if not held(job):
            return
        pair, places, _ = jobs[job]
        for half in (0, 1):
            at = (pair, *part_of(2 if half == 0 else 1), halves[half], z_range(job), places)
            first_copy(job, half, 1).wait_recv()
            mates[at] = mates[at] + first_in[pair, half, 1, :, z_range(job), places]
            second_copy(job, half).start()

    def second_finish(job):
        if not held(job):
            return
        pair, places, _ = jobs[job]
        for half in (0, 1):
            at = (pair, s_y, s_x, halves[half], z_range(job), places)
            first_copy(job, half, 0).wait_recv()
            second_copy(job, half).wait_recv()
            mates[at] = (
                mates[at]
                + first_in[pair, half, 0, :, z_range(job), places]
                + second_in[pair, half, :, z_range(job), places]
            )

    def last_start(job):
        if not held(job):
            return
        for mask in last_masks(job):
            last_copy(job, mask).start()

    def last_finish(job):
        if not held(job):
            return
        pair, places, _ = jobs[job]
        total = mates[pair, s_y, s_x, z_hi, z_lo, places]
        for mask in last_masks(job):
            last_copy(job, mask).wait_recv()
            total = total + last_in[pair, mask, places]
        out_ref[pair, places] = total

    pair01, pair02, pair12 = 0, 1, 2
    arrive(0)
    build(0)
    arrive(1)
    build(1)
    by_columns(acc_a, True, ((1, 0, 1), (-1, 1, 0)))
    pack(acc_a, pair01)
    by_columns(acc_b, True, ((1, 0, 2),))
    mates_finish(pair01)
    by_columns(acc_a, True, ((1, 1, 2),))
    first_finish(whole01)
    second_finish(whole01)

    arrive(2)
    last_start(whole01)
    build(2)
    by_columns(acc_b, False, ((-1, 2, 0),))
    pack(acc_b, pair02)
    by_columns(acc_a, False, ((-1, 2, 1),), 0, EARLY)
    mates_finish(pair02)
    by_columns(acc_a, False, ((-1, 2, 1),), EARLY)
    first_finish(plain02)
    pack(acc_a, pair12)
    mates_finish(pair12)
    low_finish(low02)
    second_finish(plain02)
    last_start(plain02)
    first_finish(plain12)
    for mask in PARTS:
        first_start(more12, mask)
    first_finish(low02)
    low_finish(low12)
    second_finish(plain12)
    last_start(plain12)
    first_finish(more12)
    second_finish(low02)
    last_start(low02)
    first_finish(low12)
    second_finish(more12)
    last_start(more12)
    second_finish(low12)
    last_start(low12)
    last_finish(whole01)
    last_finish(plain02)
    last_finish(low02)
    last_finish(plain12)
    last_finish(more12)
    last_finish(low12)

    for mask in order:
        amp_copy(0, mask).wait_send()
        amp_copy(1, mask).wait_send()
        amp_copy(2, mask).wait_send()
    for job, (_, _, low) in enumerate(jobs):
        if not held(job):
            continue
        for mask in PARTS:
            if low:
                low_copy(job, mask).wait_send()
        for half in (0, 1):
            for far in (0, 1):
                first_copy(job, half, far).wait_send()
            second_copy(job, half).wait_send()
        for mask in last_masks(job):
            last_copy(job, mask).wait_send()


def local(amplitudes, integrals, slot_tile):
    n_slab = lax.axis_size("slab")
    n_blk = lax.axis_size("blk")
    n_out, slot_dev, tile_len = amplitudes.shape[1:4]
    v_width = integrals.shape[-1]
    blocks = (v_width + tile_len - 1) // tile_len
    padded = blocks * tile_len
    row_part = tile_len // n_slab
    n_z = n_blk // 2
    half_hi = n_z // 4
    n_jobs = 6
    assert n_slab == 4 and n_out == 3 and n_blk & (n_blk - 1) == 0 and n_blk >= 8 and slot_dev > 1
    bf16, f32 = amplitudes.dtype, jnp.float32
    piece = (slot_dev, row_part, tile_len)
    dma = pltpu.SemaphoreType.DMA
    n_slots = slot_tile.shape[0]
    slot_ids = jnp.arange(n_slots, dtype=jnp.int32)
    tile_ids = jnp.arange(blocks * blocks, dtype=jnp.int32)
    slot_of = jnp.sum(jnp.where(slot_tile[None] == tile_ids[:, None], slot_ids[None], 0), axis=1)
    dims = (n_slab, n_blk, blocks, v_width, slot_dev, tile_len)
    return pl.pallas_call(
        functools.partial(cycle_kernel, dims),
        out_shape=jax.ShapeDtypeStruct((n_out,) + piece, f32),
        in_specs=[
            pl.BlockSpec(memory_space=pltpu.SMEM),
            pl.BlockSpec(memory_space=pltpu.SMEM),
            pl.BlockSpec(memory_space=pl.ANY),
            pl.BlockSpec(memory_space=pl.ANY),
        ],
        out_specs=pl.BlockSpec(memory_space=pltpu.VMEM),
        scratch_shapes=[pltpu.VMEM((n_blk, slot_dev, tile_len, tile_len), bf16)] * 3
        + [pltpu.VMEM((padded, padded), bf16)] * 3
        + [
            pltpu.VMEM((2, row_chunk(v_width), v_width), bf16),
            pltpu.VMEM((3, padded, padded), bf16),
            pltpu.VMEM((blocks, blocks, tile_len, tile_len), f32),
            pltpu.VMEM((blocks, blocks, tile_len, tile_len), f32),
            pltpu.VMEM((2, 2, 2, n_z // 2, 2) + piece, f32),
            pltpu.VMEM((3, 2, 2, n_z // 2, 2) + piece, f32),
            pltpu.VMEM((3, 2, 2, n_z // 2) + piece, f32),
            pltpu.VMEM((3, 2, 2, half_hi, 2) + piece, f32),
            pltpu.VMEM((3, 2, half_hi, 2) + piece, f32),
            pltpu.VMEM((3, n_z) + piece, f32),
            dma((2,)),
            dma((3,)),
            dma((3, n_blk)),
            dma((3, n_blk)),
            dma((3, 4)),
            dma((3, 4)),
            dma((n_jobs, 4)),
            dma((n_jobs, 4)),
            dma((n_jobs, 2, 2)),
            dma((n_jobs, 2, 2)),
            dma((n_jobs, 2)),
            dma((n_jobs, 2)),
            dma((n_jobs, n_z)),
            dma((n_jobs, n_z)),
        ],
        compiler_params=pltpu.CompilerParams(
            collective_id=0, has_side_effects=True, vmem_limit_bytes=67043328
        ),
        name="cycle",
    )(slot_of, slot_tile, amplitudes, integrals)


def solution(mesh):
    return jax.shard_map(
        local,
        mesh=mesh,
        in_specs=(P("slab", None, "blk", None, None), P(("slab", "blk"), None, None, None), P()),
        out_specs=P(None, "blk", "slab", None),
        check_vma=False,
    )
```
